32 devices in a mesh: gx: 8 (over z, x), gy: 4 (over y, core).
Axes of the slice: x: 2, y: 2, z: 4, core: 2. Of those that a mesh axis runs over, the one named last changes fastest.
Arguments:
- image: float32 [32, 128, 512], P(None, 'gx', 'gy'), may hold values from -6 to 6
Outputs:
- likelihood: float32 [32, 128, 512], P(None, 'gx', 'gy')
The draws below stay inside these ranges and needn't reach their ends.
All inputs are finite; a program needn't handle non-finite values.
Results may differ from the reference program's by a relative error of at most 0.0003.
Values sent between devices are 32-bit elements; how exact they have to be, the bound alone decides.
A program may use at most 64 MiB of HBM per device.

```python
import jax
import jax.numpy as jnp
from jax import lax

DEPTH = 32
DIP_HALF = 4
STRIKE_HALF = 8
NX = 128
NY = 512
N_GX = 8


def shard_levels(stream_key, extent, shards, smallest, high):
    def one(axis_at, blocks):
        heights = jax.random.uniform(jax.random.fold_in(jax.random.fold_in(stream_key, 6), axis_at), (blocks,), jnp.float32, smallest / len(shards), high / len(shards))
        return jnp.repeat(jnp.exp(heights), extent[axis_at] // blocks).reshape((-1,) + (1,) * (len(extent) - axis_at - 1))

    factor_of = one(*shards[0])
    for cut in shards[1:]:
        factor_of = factor_of * one(*cut)
    return factor_of


def noise(own_key, extent, scale, reach, pieces=(), kind=jnp.bfloat16):
    values = jax.random.normal(own_key, extent, jnp.float32) * scale
    if len(pieces) > 0:
        values = shard_levels(own_key, extent, pieces, -0.22, 0.18) * values
    return jnp.clip(values, min=-reach, max=reach).astype(kind)


def setup_inputs(seed: int = 0) -> dict:
    splits = jax.random.split(jax.random.key(seed), 2)
    return {
        "image": noise(splits[0], (DEPTH, NX, NY), 1.0, 6.0, ((1, 8), (2, 4)), jnp.float32),
    }


EPSILON = 1e-6


def dip_sums(volume, squares, incline, normal, margin, normal_count):
    samples = volume.shape[0] - 2 * DIP_HALF
    amp_total = jnp.zeros((), jnp.float32)
    power_total = jnp.zeros((), jnp.float32)
    for offset in range(-DIP_HALF, DIP_HALF + 1):
        start = margin + incline * offset
        rows_a = lax.slice_in_dim(volume, DIP_HALF + offset, DIP_HALF + offset + samples, axis=0)
        rows_p = lax.slice_in_dim(squares, DIP_HALF + offset, DIP_HALF + offset + samples, axis=0)
        amp_total = amp_total + lax.slice_in_dim(rows_a, start, start + normal_count, axis=normal)
        power_total = power_total + lax.slice_in_dim(rows_p, start, start + normal_count, axis=normal)
    return amp_total, power_total


def strike_sum(values, strike, margin, strike_count):
    total = jnp.zeros((), jnp.float32)
    for offset in range(-STRIKE_HALF, STRIKE_HALF + 1):
        total = total + lax.slice_in_dim(values, margin + offset, margin + offset + strike_count, axis=strike)
    return total


def largest_likely(extended, margin, count_x, count_y):
    volume = jnp.pad(extended, ((DIP_HALF, DIP_HALF), (0, 0), (0, 0)))
    squares = volume * volume
    largest = None
    for normal, strike, normal_count, strike_count in ((1, 2, count_x, count_y), (2, 1, count_y, count_x)):
        for incline in (-1, 0, 1):
            amp, power = dip_sums(volume, squares, incline, normal, margin, normal_count)
            numerator = strike_sum(amp * amp, strike, margin, strike_count)
            denominator = strike_sum(power, strike, margin, strike_count)
            likely = 1.0 - numerator / ((2 * DIP_HALF + 1) * denominator + EPSILON)
            largest = likely if largest is None else jnp.maximum(largest, likely)
    return largest


def reference(image):
    margin = max(DIP_HALF, STRIKE_HALF)
    padded = jnp.pad(image, ((0, 0), (margin, margin), (margin, margin)))
    block_rows = NX // N_GX

    def one_block(block_index):
        start = (block_index * block_rows).astype(jnp.int32)
        extended = lax.dynamic_slice_in_dim(padded, start, block_rows + 2 * margin, axis=1)
        return largest_likely(extended, margin, block_rows, NY)

    blocks = lax.map(one_block, jnp.arange(N_GX, dtype=jnp.int32))
    return jnp.moveaxis(blocks, 0, 1).reshape(DEPTH, NX, NY)
```

```python
import functools

import jax
import jax.numpy as jnp
from jax import lax
from jax.experimental import pallas as pl
from jax.experimental.pallas import tpu as pltpu
from jax.sharding import PartitionSpec as P

DIP_HALF = 4
STRIKE_HALF = 8
EPSILON = 1e-06
LANES = 128
TILE = 8
CHUNK = 8
F32 = jnp.float32


def band_matrix():
    position = lax.broadcasted_iota(jnp.int32, (2 * LANES, LANES), 0)
    position = jnp.where(position < LANES + LANES // 2, position, position - 2 * LANES)
    distance = position - lax.broadcasted_iota(jnp.int32, (2 * LANES, LANES), 1)
    return jnp.where(jnp.abs(distance) <= STRIKE_HALF, 1.0, 0.0).astype(jnp.bfloat16)


def band_sum(values, band):
    high = values.astype(jnp.bfloat16)
    low = (values - high.astype(F32)).astype(jnp.bfloat16)
    return jnp.dot(high, band, preferred_element_type=F32) + jnp.dot(
        low, band, preferred_element_type=F32
    )


def ring_roll(main, halo, z, left, both):
    lane = lax.broadcasted_iota(jnp.int32, main.shape, 1)
    if left:
        shift = lax.rem(LANES - z, LANES)
        keep = lane < LANES - z
    else:
        shift = z
        keep = lane >= z
    main = pltpu.roll(main, shift, 1)
    halo = pltpu.roll(halo, shift, 1)
    moved = jnp.where(keep, main, halo)
    return (moved, jnp.where(keep, halo, main)) if both else moved


def row_windows(rows, count):
    total = rows.shape[0]
    width = rows
    for step in (1, 2, 4):
        width = width + pltpu.roll(width, total - step, 0)
    return (
        width[:count] + width[STRIKE_HALF : STRIKE_HALF + count]
        + rows[2 * STRIKE_HALF : 2 * STRIKE_HALF + count]
    )


def dip_window(planes):
    two = [a + b for a, b in zip(planes[:-1], planes[1:])]
    four = [a + b for a, b in zip(two[:-2], two[2:])]
    eight = [a + b for a, b in zip(four[:-4], four[4:])]
    return [a + b for a, b in zip(eight[:CHUNK], planes[8:])]


def column(ref, base, first, rows):
    return [ref[base + j, pl.ds(first, rows), :] for j in range(CHUNK + 2 * DIP_HALF)]


def prepare_own(chunk, rows, main_ref, halo_ref, box_ref, shear_refs, band):
    own = rows - 2 * STRIKE_HALF
    at = pl.ds(STRIKE_HALF, own)
    base = chunk * CHUNK
    squares = []
    for i in range(CHUNK):
        z = base + i
        main = main_ref[z + DIP_HALF, at, :]
        halo = halo_ref[z + DIP_HALF, at, :]
        squares.append(jnp.concatenate([main * main, halo * halo], axis=1))
        for left, (s_main, s_halo) in ((True, shear_refs[0]), (False, shear_refs[1])):
            s_main[z + DIP_HALF, at, :], s_halo[z + DIP_HALF, at, :] = ring_roll(
                main, halo, z, left, True
            )
    boxed = band_sum(jnp.concatenate(squares, axis=0), band)
    for i in range(CHUNK):
        box_ref[base + i + DIP_HALF, at, :] = boxed[i * own : (i + 1) * own]


def ratio(numerator, denominator):
    return numerator / ((2 * DIP_HALF + 1) * denominator + EPSILON)


def sheared_squares(s_main, s_halo, base, firsts, left):
    tiles = [
        (dip_window(column(s_main, base, t, TILE)), dip_window(column(s_halo, base, t, TILE)))
        for t in firsts
    ]
    result = []
    for i in range(CHUNK):
        amp = ring_roll(
            jnp.concatenate([tile[0][i] for tile in tiles], axis=0),
            jnp.concatenate([tile[1][i] for tile in tiles], axis=0),
            base + i, not left, False,
        )
        result.append(amp * amp)
    return result


def finish_own(chunk, rows, main_ref, halo_ref, box_ref, shear_refs, square_refs, band, out_ref):
    own = rows - 2 * STRIKE_HALF
    first = STRIKE_HALF
    base = chunk * CHUNK
    squares = [[], []]
    for ref, into in ((main_ref, squares[0]), (halo_ref, squares[1])):
        tiles = [dip_window(column(ref, base, t, TILE)) for t in range(first, first + own, TILE)]
        for i in range(CHUNK):
            amp = jnp.concatenate([tile[i] for tile in tiles], axis=0)
            into.append(amp * amp)
    for i in range(CHUNK):
        square_refs[0][base + i] = squares[0][i]
    numerators = band_sum(
        jnp.concatenate([jnp.concatenate(pair, axis=1) for pair in zip(*squares)], axis=0), band
    )
    denominators = dip_window(column(box_ref, base, first, own))
    for i in range(CHUNK):
        out_ref[base + i] = ratio(numerators[i * own : (i + 1) * own], denominators[i])
    for left, (s_main, s_halo), square in (
        (True, shear_refs[0], square_refs[1]), (False, shear_refs[1], square_refs[2])
    ):
        values = sheared_squares(s_main, s_halo, base, range(first, first + own, TILE), left)
        for i in range(CHUNK):
            square[base + i] = values[i]


def prepare(chunk, rows, main_ref, halo_ref, box_ref, row_ref, shear_refs, shear_row_refs, band):
    own = rows - 2 * STRIKE_HALF
    w = STRIKE_HALF
    base = chunk * CHUNK
    squares = []

    def edges(values):
        return jnp.concatenate([values[:w], values[w + own :]], axis=0)

    for i in range(CHUNK):
        z = base + i
        main = main_ref[z + DIP_HALF]
        halo = halo_ref[z + DIP_HALF]
        main_sq = main * main
        halo_sq = halo * halo
        squares.append(jnp.concatenate([edges(main_sq), edges(halo_sq)], axis=1))
        main_row = row_windows(main_sq, own)
        halo_row = row_windows(halo_sq, own)
        row_ref[z + DIP_HALF] = main_row
        for left, (s_main, s_halo), (r_main, r_halo) in (
            (True, shear_refs[0], shear_row_refs[0]),
            (False, shear_refs[1], shear_row_refs[1]),
        ):
            a, b = ring_roll(edges(main), edges(halo), z, left, True)
            for ref, value in ((s_main, a), (s_halo, b)):
                ref[z + DIP_HALF, pl.ds(0, w), :] = value[:w]
                ref[z + DIP_HALF, pl.ds(w + own, w), :] = value[w:]
            a, b = ring_roll(main_row, halo_row, z, left, True)
            r_main[z + DIP_HALF] = a
            r_halo[z + DIP_HALF] = b
    boxed = band_sum(jnp.concatenate(squares, axis=0), band)
    for i in range(CHUNK):
        at = i * 2 * w
        box_ref[base + i + DIP_HALF, pl.ds(0, w), :] = boxed[at : at + w]
        box_ref[base + i + DIP_HALF, pl.ds(w + own, w), :] = boxed[at + w : at + 2 * w]


def finish(
    chunk, rows, main_ref, halo_ref, box_ref, row_ref, shear_refs, shear_row_refs, square_refs,
    band, out_ref,
):
    own = rows - 2 * STRIKE_HALF
    base = chunk * CHUNK
    first = STRIKE_HALF
    best = [out_ref[base + i] for i in range(CHUNK)]

    def combine(i, numerator, denominator):
        best[i] = jnp.minimum(best[i], ratio(numerator, denominator))

    def sloped(ref, i, incline):
        total = None
        for d in range(-DIP_HALF, DIP_HALF + 1):
            term = ref[base + i + DIP_HALF + d, pl.ds(first + incline * d, own), :]
            total = term if total is None else total + term
        return total

    top = dip_window(column(main_ref, base, 0, first))
    bottom = dip_window(column(main_ref, base, first + own, first))
    denominators = dip_window(column(row_ref, base, 0, own))
    for i in range(CHUNK):
        amp_sq = jnp.concatenate(
            [top[i] * top[i], square_refs[0][base + i], bottom[i] * bottom[i]], axis=0
        )
        combine(i, row_windows(amp_sq, own), denominators[i])

    for incline in (-1, 1):
        squares = []
        for i in range(CHUNK):
            amp = sloped(main_ref, i, incline)
            halo = sloped(halo_ref, i, incline)
            squares.append(jnp.concatenate([amp * amp, halo * halo], axis=1))
        numerators = band_sum(jnp.concatenate(squares, axis=0), band)
        for i in range(CHUNK):
            combine(i, numerators[i * own : (i + 1) * own], sloped(box_ref, i, incline))

    for left, (s_main, s_halo), (r_main, r_halo), square in (
        (True, shear_refs[0], shear_row_refs[0], square_refs[1]),
        (False, shear_refs[1], shear_row_refs[1], square_refs[2]),
    ):
        values = sheared_squares(s_main, s_halo, base, (0, first + own), left)
        row_tiles = [
            (dip_window(column(r_main, base, t, TILE)), dip_window(column(r_halo, base, t, TILE)))
            for t in range(0, own, TILE)
        ]
        for i in range(CHUNK):
            denominator = ring_roll(
                jnp.concatenate([tile[0][i] for tile in row_tiles], axis=0),
                jnp.concatenate([tile[1][i] for tile in row_tiles], axis=0),
                base + i, not left, False,
            )
            amp_sq = jnp.concatenate(
                [values[i][:first], square[base + i], values[i][first:]], axis=0
            )
            combine(i, row_windows(amp_sq, own), denominator)

    for i in range(CHUNK):
        out_ref[base + i] = best[i]


SIDE = STRIKE_HALF
GROUP = LANES // SIDE
MESH = pl.DeviceIdType.MESH


def kernel(
    count_x, count_y, image_ref, out_ref, main, halo, box, row,
    sl_m, sl_h, sr_m, sr_h, rl_m, rl_h, rr_m, rr_h, square_0, square_1, square_2,
    pack_first, pack_last, after, before, send_x, recv_x, send_s, recv_s, load_sem,
):
    depth, own, _ = image_ref.shape
    rows = own + 2 * STRIKE_HALF
    chunks = depth // CHUNK
    w = STRIKE_HALF
    body = pl.ds(DIP_HALF, depth)
    mine = main.at[body, pl.ds(w, own), :]
    load = pltpu.make_async_copy(image_ref, mine, load_sem)
    load.start()
    gx = lax.axis_index("gx")
    gy = lax.axis_index("gy")
    exists = {
        (dx, dy): jnp.logical_and(
            jnp.logical_and(gx + dx >= 0, gx + dx < count_x),
            jnp.logical_and(gy + dy >= 0, gy + dy < count_y),
        )
        for dx in (-1, 0, 1) for dy in (-1, 0, 1) if (dx, dy) != (0, 0)
    }

    def device(dx, dy):
        return (lax.rem(gx + dx + count_x, count_x), lax.rem(gy + dy + count_y, count_y))

    edge = jnp.zeros((depth, w, LANES), F32)
    main[body, pl.ds(0, w), :] = edge
    main[body, pl.ds(w + own, w), :] = edge
    after[...] = jnp.zeros(after.shape, F32)
    before[...] = jnp.zeros(before.shape, F32)
    barrier = pltpu.get_barrier_semaphore()
    faces = {key: there for key, there in exists.items() if 0 in key}
    for (dx, dy), there in faces.items():
        @pl.when(there)
        def _(dx=dx, dy=dy):
            pl.semaphore_signal(barrier, inc=1, device_id=device(dx, dy), device_id_type=MESH)

    for ref in (main, halo, box, row, sl_m, sl_h, sr_m, sr_h, rl_m, rl_h, rr_m, rr_h):
        zeros = jnp.zeros((DIP_HALF,) + ref.shape[1:], F32)
        ref[pl.ds(0, DIP_HALF)] = zeros
        ref[pl.ds(depth + DIP_HALF, DIP_HALF)] = zeros
    load.wait()

    lane = lax.broadcasted_iota(jnp.int32, (own, LANES), 1)
    for q in range(depth // GROUP):
        first = main[q * GROUP + DIP_HALF, pl.ds(w, own), :]
        last = pltpu.roll(main[q * GROUP + DIP_HALF, pl.ds(w, own), :], SIDE, 1)
        for j in range(1, GROUP):
            plane = main[q * GROUP + j + DIP_HALF, pl.ds(w, own), :]
            first = jnp.where(lane >= SIDE * j, pltpu.roll(plane, SIDE * j, 1), first)
            last = jnp.where(
                lane >= SIDE * j, pltpu.roll(plane, (SIDE * j + SIDE) % LANES, 1), last
            )
        pack_first[q] = first
        pack_last[q] = last

    band = band_matrix()

    def side_copy(index, dx, dy):
        source, target = (pack_first, after) if dy < 0 else (pack_last, before)
        at, length, to = {0: (0, own, w), -1: (w, w, w + own), 1: (own, w, 0)}[dx]
        if dx != 0:
            source = target
        return pltpu.make_async_remote_copy(
            src_ref=source.at[:, pl.ds(at, length), :],
            dst_ref=target.at[:, pl.ds(to, length), :],
            send_sem=send_s.at[index], recv_sem=recv_s.at[index],
            device_id=device(dx, 0 if dx else dy), device_id_type=MESH,
        )

    def row_copy(index, dx, chunk):
        at, to = (0, w + own) if dx < 0 else (own - w, 0)
        return pltpu.make_async_remote_copy(
            src_ref=main.at[pl.ds(chunk * CHUNK + DIP_HALF, CHUNK), pl.ds(w + at, w), :],
            dst_ref=main.at[pl.ds(chunk * CHUNK + DIP_HALF, CHUNK), pl.ds(to, w), :],
            send_sem=send_x.at[index, chunk], recv_sem=recv_x.at[index, chunk],
            device_id=device(dx, 0), device_id_type=MESH,
        )

    sides = [(0, -1), (0, 1), (-1, -1), (-1, 1), (1, -1), (1, 1)]
    expected = sum(jnp.where(there, 1, 0) for there in faces.values())
    pl.semaphore_wait(barrier, expected)
    def send_sides(corners):
        for index, (dx, dy) in enumerate(sides):
            if (dx != 0) == corners:
                @pl.when(exists[dx, -dy] if corners else exists[dx, dy])
                def _(index=index, dx=dx, dy=dy):
                    side_copy(index, dx, dy).start()

    def send_rows(first, last):
        for chunk in range(first, last):
            for index, dx in enumerate((-1, 1)):
                @pl.when(exists[dx, 0])
                def _(index=index, dx=dx, chunk=chunk):
                    row_copy(index, dx, chunk).start()

    send_rows(0, chunks // 2)
    send_sides(False)

    def arrive(corners):
        for index, (dx, dy) in enumerate(sides):
            if (dx != 0) == corners:
                @pl.when(exists[-dx, -dy])
                def _(index=index, dx=dx, dy=dy):
                    side_copy(index, dx, dy).wait_recv()

    def unpack(at, length):
        lane = lax.broadcasted_iota(jnp.int32, (length, LANES), 1)
        for q in range(depth // GROUP):
            right = after[q, pl.ds(at, length), :]
            left = before[q, pl.ds(at, length), :]
            for j in range(GROUP):
                a = pltpu.roll(right, (LANES - SIDE * j) % LANES, 1)
                b = pltpu.roll(left, (2 * LANES - SIDE - SIDE * j) % LANES, 1)
                halo[q * GROUP + j + DIP_HALF, pl.ds(at, length), :] = jnp.where(
                    lane < SIDE, a, jnp.where(lane >= LANES - SIDE, b, 0.0)
                )

    arrive(False)
    send_sides(True)
    send_rows(chunks // 2, chunks - 1)
    unpack(w, own)
    send_rows(chunks - 1, chunks)

    shear = ((sl_m, sl_h), (sr_m, sr_h))
    shear_row = ((rl_m, rl_h), (rr_m, rr_h))

    squares = (square_0, square_1, square_2)

    @pl.loop(0, chunks + 1)
    def _(chunk):
        @pl.when(chunk < chunks)
        def _():
            prepare_own(chunk, rows, main, halo, box, shear, band)

        @pl.when(chunk > 0)
        def _():
            finish_own(chunk - 1, rows, main, halo, box, shear, squares, band, out_ref)

    arrive(True)
    unpack(0, w)
    unpack(w + own, w)

    @pl.loop(0, chunks + 1)
    def _(chunk):
        @pl.when(chunk < chunks)
        def _():
            for index, dx in enumerate((-1, 1)):
                @pl.when(exists[-dx, 0])
                def _(index=index, dx=dx):
                    row_copy(index, dx, chunk).wait_recv()
            prepare(chunk, rows, main, halo, box, row, shear, shear_row, band)

        @pl.when(chunk > 0)
        def _():
            finish(chunk - 1, rows, main, halo, box, row, shear, shear_row, squares, band, out_ref)

    for index, (dx, dy) in enumerate(sides):
        @pl.when(exists[dx, -dy] if dx else exists[dx, dy])
        def _(index=index, dx=dx, dy=dy):
            side_copy(index, dx, dy).wait_send()
    for chunk in range(chunks):
        for index, dx in enumerate((-1, 1)):
            @pl.when(exists[dx, 0])
            def _(index=index, dx=dx, chunk=chunk):
                row_copy(index, dx, chunk).wait_send()


def shards(image):
    depth, own, width = image.shape
    rows = own + 2 * STRIKE_HALF
    planes = depth + 2 * DIP_HALF
    full = pltpu.VMEM((planes, rows, LANES), F32)
    part = pltpu.VMEM((planes, own, LANES), F32)
    groups = depth // GROUP
    semblance = pl.pallas_call(
        functools.partial(kernel, lax.axis_size("gx"), lax.axis_size("gy")),
        out_shape=jax.ShapeDtypeStruct(image.shape, F32),
        in_specs=[pl.BlockSpec(memory_space=pltpu.HBM)],
        out_specs=pl.BlockSpec(memory_space=pltpu.VMEM),
        scratch_shapes=[full, full, full, part] + [full] * 4 + [part] * 4
        + [pltpu.VMEM(image.shape, F32)] * 3
        + [pltpu.VMEM((groups, own, LANES), F32)] * 2
        + [pltpu.VMEM((groups, rows, LANES), F32)] * 2
        + [pltpu.SemaphoreType.DMA((2, depth // CHUNK))] * 2
        + [pltpu.SemaphoreType.DMA((6,))] * 2 + [pltpu.SemaphoreType.DMA],
        compiler_params=pltpu.CompilerParams(
            vmem_limit_bytes=40 * 1024 * 1024, collective_id=0, has_side_effects=True
        ),
    )(pltpu.with_memory_space_constraint(image, pltpu.HBM))
    return 1.0 - semblance


def solution(mesh):
    spec = P(None, "gx", "gy")
    return jax.shard_map(shards, mesh=mesh, in_specs=(spec,), out_specs=spec, check_vma=False)
```
